32 devices in a mesh: gx: 4 (over y, x), gy: 8 (over z, core).
Axes of the slice: x: 2, y: 2, z: 4, core: 2. Of those that a mesh axis runs over, the one named last changes fastest.
Arguments:
- embeddings: bfloat16 [163840, 1024], P(('gx', 'gy')), may hold values from -6 to 6
- device_local_selections: int32 [32, 64], P(('gx', 'gy')), may hold values from 0 to 5119
- merge_picks: int32 [32, 64], replicated, may hold values from 0 to 127
Outputs:
- final_centers: bfloat16 [64, 1024], replicated
- coverage: float32 [163840], P(('gx', 'gy'))
- radius: float32 [], replicated
The draws below stay inside these ranges and needn't reach their ends.
All inputs are finite; a program needn't handle non-finite values.
Results may differ from the reference program's by a relative error of at most 0.001.
Values may be sent and summed in bfloat16 or wider, within the bound.
No kernel may reach another device: no remote copies, remote signals or barrier semaphores. Data moves between devices by JAX's collectives and lax.ppermute only.
A program may use at most 64 MiB of HBM per device.

```python
import jax
import jax.numpy as jnp
from jax import lax

D = 1024
CENTERS = 64
ROWS_DEV = 5120
MERGED = 128
POINTS = 163840
DEVICES = 32


def set_ends(entries, key, least, largest):
    dims = entries.shape
    index_at = [jax.random.randint(jax.random.fold_in(key, axis), (), 0, dims[axis]) for axis in range(len(dims))]
    entries = entries.at[tuple(index_at)].set(least)
    longest = dims.index(max(dims))
    index_at[longest] = (index_at[longest] + 1) % dims[longest]
    return entries.at[tuple(index_at)].set(largest)


def shard_levels(own_key, extent, split, smallest, high):
    def one(axis_at, parts):
        steps = jax.random.uniform(jax.random.fold_in(jax.random.fold_in(own_key, 6), axis_at), (parts,), jnp.float32, smallest / len(split), high / len(split))
        return jnp.repeat(jnp.exp(steps), extent[axis_at] // parts).reshape((-1,) + (1,) * (len(extent) - axis_at - 1))

    gain = one(*split[0])
    for cut in split[1:]:
        gain = gain * one(*cut)
    return gain


def scatter_about(rng, shape, spread, limit, pieces=(), kind=jnp.bfloat16):
    array = spread * jax.random.normal(rng, shape, jnp.float32)
    if pieces:
        array = array * shard_levels(rng, shape, pieces, -0.22, 0.18)
    return jnp.clip(array, -limit, limit).astype(kind)


def setup_inputs(seed: int = 0) -> dict:
    splits = jax.random.split(jax.random.key(seed), 4)
    return {
        "embeddings": scatter_about(splits[0], (POINTS, D), 1.0, 6.0, ((0, 32),)),
        "device_local_selections": set_ends(jax.random.randint(splits[1], (DEVICES, CENTERS), 0, ROWS_DEV), jax.random.fold_in(splits[1], 1), 0, ROWS_DEV - 1).astype(jnp.int32),
        "merge_picks": set_ends(jax.random.randint(splits[2], (DEVICES, CENTERS), 0, MERGED), jax.random.fold_in(splits[2], 1), 0, MERGED - 1).astype(jnp.int32),
    }


def nearest(points, squares, chosen_centroids):
    wide = chosen_centroids.astype(jnp.float32)
    csq = jnp.sum(wide * wide, axis=1)
    prod = jnp.dot(points, chosen_centroids.T, preferred_element_type=jnp.float32)
    return jnp.min(squares[:, None] - 2.0 * prod + csq[None, :], axis=1) / D


def reference(embeddings, device_local_selections, merge_picks):
    devices = DEVICES
    rounds = devices.bit_length() - 1
    points = embeddings.reshape(devices, ROWS_DEV, D)
    squares = jnp.sum(points.astype(jnp.float32) ** 2, axis=2)
    sets = jnp.take_along_axis(points, device_local_selections[:, :, None], axis=1)
    cover = lax.map(lambda a: nearest(a[0], a[1], a[2]), (points, squares, sets))
    ident = jnp.arange(devices, dtype=jnp.int32)
    for step in range(rounds):
        partner = ident ^ (1 << step)
        other = sets[partner]
        cover = jnp.minimum(cover, lax.map(lambda a: nearest(a[0], a[1], a[2]), (points, squares, other)))
        lower = (((ident >> step) & 1) == 0)[:, None, None]
        first = jnp.where(lower, sets, other)
        latter_half = jnp.where(lower, other, sets)
        combined_selection = jnp.concatenate([first, latter_half], axis=1)
        rows = (devices - (devices >> step) + (ident >> (step + 1))).astype(jnp.int32)
        selected_indices = merge_picks[rows]
        sets = jnp.take_along_axis(combined_selection, selected_indices[:, :, None], axis=1)
    return sets[0], cover.reshape(-1), jnp.max(cover)
```

```python
import jax
import jax.numpy as jnp
from jax import lax
from jax.sharding import PartitionSpec as P


def swapped(value, axis, distance):
    mask = 2**distance
    pairs = [(source, source ^ mask) for source in range(lax.axis_size(axis))]
    return lax.ppermute(value, axis, pairs)


def nearest(points, squares, chosen_centroids, width):
    wide = chosen_centroids.astype(jnp.float32)
    csq = jnp.sum(wide * wide, axis=1)
    prod = jnp.dot(points, chosen_centroids.T, preferred_element_type=jnp.float32)
    return jnp.min(squares[:, None] - 2.0 * prod + csq[None, :], axis=1) / width


def choose_again(combined_selection, selected_indices, center_count):
    onehot = (
        lax.broadcasted_iota(jnp.int32, (selected_indices.shape[0], center_count), 1)
        == selected_indices[:, None]
    ).astype(jnp.bfloat16)
    return jnp.dot(onehot, combined_selection, preferred_element_type=jnp.float32).astype(
        jnp.bfloat16
    )


def per_device(embeddings, device_local_selections, merge_picks):
    rows, width = embeddings.shape
    chosen_centroids = device_local_selections.shape[1]
    size_gx = lax.axis_size("gx")
    size_gy = lax.axis_size("gy")
    devices = size_gx * size_gy
    index_gx = lax.axis_index("gx")
    index_gy = lax.axis_index("gy")
    mine = index_gx * size_gy + index_gy
    onehot = (
        lax.broadcasted_iota(jnp.int32, (chosen_centroids, rows), 1)
        == device_local_selections[0][:, None]
    ).astype(jnp.bfloat16)
    sets = jnp.dot(onehot, embeddings, preferred_element_type=jnp.float32).astype(jnp.bfloat16)
    wide = embeddings.astype(jnp.float32)
    squares = jnp.sum(wide * wide, axis=1)
    seen = [sets]
    cover = nearest(embeddings, squares, sets, width)

    def account(cover, other):
        seen.append(other)
        return cover

    def combine(sets, other, step, number):
        lower = number >> step & 1 == 0
        combined_selection = jnp.where(
            lower, jnp.concatenate([sets, other], 0), jnp.concatenate([other, sets], 0)
        )
        row = devices - (devices >> step) + (number >> step + 1)
        selected_indices = lax.dynamic_index_in_dim(merge_picks, row, 0, keepdims=False)
        return choose_again(combined_selection, selected_indices, 2 * chosen_centroids)

    bits_gy = size_gy.bit_length() - 1
    horizontal_grid_bits = size_gx.bit_length() - 1
    for step in range(bits_gy):
        other = swapped(sets, "gy", step)
        cover = account(cover, other)
        sets = combine(sets, other, step, mine)
    for level in range(horizontal_grid_bits):
        step = bits_gy + level
        other = swapped(sets, "gx", level)
        cover = account(cover, other)
        sets = combine(sets, other, step, mine)
    cover = nearest(embeddings, squares, jnp.concatenate(seen, axis=0), width)
    peak = jnp.broadcast_to(jnp.max(cover), (8, 128))
    bit = 1
    while bit < devices:
        mask = bit | 1
        pairs = [(source, source ^ mask) for source in range(devices)]
        peak = jnp.maximum(peak, lax.ppermute(peak, ("gx", "gy"), pairs))
        bit *= 2
    return (sets, cover, peak[0, 0])


def solution(mesh):
    return jax.shard_map(
        per_device,
        mesh=mesh,
        in_specs=(P(("gx", "gy"), None), P(("gx", "gy"), None), P()),
        out_specs=(P(), P(("gx", "gy")), P()),
        check_vma=False,
    )
```

```python
import functools

import jax
import jax.numpy as jnp
from jax import lax
from jax.experimental import pallas as pl
from jax.experimental.pallas import tpu as pltpu
from jax.sharding import PartitionSpec as P


GROUP = 8
CHUNK = 256
FAR = 3.0e38
NT = (((1,), (1,)), ((), ()))
VMEM = pl.BlockSpec(memory_space=pltpu.VMEM)


def cost(flops):
    return pl.CostEstimate(flops=flops, bytes_accessed=2**20, transcendentals=0)


def gather_kernel(picks_ref, points_ref, out_ref, held, sem):
    count = out_ref.shape[0]
    copies = []
    for i in range(count):
        start = pl.multiple_of(picks_ref[0, i] // GROUP * GROUP, GROUP)
        copies.append(
            pltpu.make_async_copy(
                points_ref.at[pl.ds(start, GROUP), :],
                held.at[pl.ds(i * GROUP, GROUP), :],
                sem.at[i],
            )
        )
        copies[-1].start()
    down = lax.broadcasted_iota(jnp.int32, (count, 128), 0)
    wanted = down * GROUP
    for i in range(count):
        wanted = jnp.where(down == i, wanted + lax.rem(picks_ref[0, i], GROUP), wanted)
    lanes = lax.broadcasted_iota(jnp.int32, (count, 128), 1)
    onehot = jnp.concatenate(
        [(lanes + base == wanted).astype(jnp.bfloat16) for base in range(0, count * GROUP, 128)],
        axis=1,
    )
    for copy in copies:
        copy.wait()
    out_ref[...] = jnp.dot(
        onehot, held[...], preferred_element_type=jnp.float32
    ).astype(jnp.bfloat16)


def gather_rows(points, picks):
    count = picks.shape[1]
    width = points.shape[1]
    return pl.pallas_call(
        gather_kernel,
        out_shape=pltpu.VMEM((count, width), points.dtype),
        in_specs=[
            pl.BlockSpec(memory_space=pltpu.SMEM),
            pl.BlockSpec(memory_space=pltpu.HBM),
        ],
        out_specs=VMEM,
        scratch_shapes=[
            pltpu.VMEM((count * GROUP, width), points.dtype),
            pltpu.SemaphoreType.DMA((count,)),
        ],
        compiler_params=pltpu.CompilerParams(vmem_limit_bytes=56 * 2**20),
        cost_estimate=cost(10**9),
        name="gather_rows",
    )(picks, points)


def swap_halves(index, count, lower):
    swapped_index = jnp.where(index < count, index + count, index - count)
    return jnp.where(lower, index, swapped_index)


def upright(row):
    size = row.shape[1]
    across = lax.broadcasted_iota(jnp.int32, (size, size), 1)
    down = lax.broadcasted_iota(jnp.int32, (size, size), 0)
    spread = jnp.where(across == down, jnp.broadcast_to(row, (size, size)), 0)
    return jnp.sum(spread.astype(jnp.float32), axis=1, keepdims=True).astype(jnp.int32)


def plan_kernel(phases, count, devices, picks_ref, *out_refs):
    number = lax.axis_index("gx") * lax.axis_size("gy") + lax.axis_index("gy")
    outs = list(out_refs)
    north = (number & 1) == 1

    def row_of(step, place):
        return picks_ref[pl.ds(devices - (devices >> step) + (place >> step + 1), 1), :]

    def onehot(column, total):
        lanes = lax.broadcasted_iota(jnp.int32, (count, total), 1)
        return (lanes == column).astype(jnp.bfloat16)

    for step, kind in phases:
        lower = (number >> step & 1) == 0
        own = swap_halves(row_of(step, number), count, lower)
        if kind == "single":
            outs.pop(0)[...] = onehot(upright(own), 2 * count)
            continue
        beside = swap_halves(row_of(step, number ^ 2 << step), count, lower)
        lower_next = (number >> step + 1 & 1) == 0
        top = upright(swap_halves(row_of(step + 1, number), count, lower_next))
        lanes = lax.broadcasted_iota(jnp.int32, (count, count), 1)
        relative = jnp.where(lanes == top, own, 0) + jnp.where(
            lanes + count == top, beside + 2 * count, 0
        )
        relative = jnp.sum(relative.astype(jnp.float32), axis=1, keepdims=True)
        relative = relative.astype(jnp.int32)
        spot = lax.broadcasted_iota(jnp.int32, (3 * count, 1), 0) + count
        if kind == "mixed":
            half = count // 2
            near = jnp.where(north, 3 * half, 0)
            far = jnp.where(north, 0, 3 * half)
            back = relative - 2 * count
            first = jnp.where(north, 0, 3 * half)
            last = jnp.where(north, 3 * half, 0) - half
            place = jnp.where(
                relative < count,
                relative,
                jnp.where(
                    relative < 2 * count,
                    relative + near,
                    jnp.where(
                        relative < 3 * count,
                        back + 2 * count + jnp.where(back < half, first, last),
                        relative - 2 * count + far,
                    ),
                ),
            )
            inside = spot - count
            second = inside >= 3 * half
            inside = jnp.where(second, inside - 3 * half, inside)
            mine = second ^ north
            spot = jnp.where(
                inside < count,
                jnp.where(mine, inside + 3 * count, inside + count),
                jnp.where(mine, inside + count, inside + count + half),
            )
        else:
            place = relative
        outs.pop(0)[...] = onehot(place, 4 * count)
        kept = jnp.where(spot - 2 * count == beside, 1.0, 0.0)
        kept = jnp.max(kept, axis=1, keepdims=True)
        kept = jnp.where(spot < 2 * count, 1.0, kept)
        outs.pop(0)[...] = jnp.where(kept > 0.5, 0.0, FAR)


def make_plan(picks, phases, devices):
    count = picks.shape[1]
    shapes = []
    for _, kind in phases:
        if kind == "single":
            shapes.append(pltpu.VMEM((count, 2 * count), jnp.bfloat16))
        else:
            shapes.append(pltpu.VMEM((count, 4 * count), jnp.bfloat16))
            shapes.append(pltpu.VMEM((3 * count, 1), jnp.float32))
    return pl.pallas_call(
        functools.partial(plan_kernel, phases, count, devices),
        out_shape=tuple(shapes),
        in_specs=[VMEM],
        out_specs=(VMEM,) * len(shapes),
        compiler_params=pltpu.CompilerParams(vmem_limit_bytes=4 * 2**20),
        cost_estimate=pl.CostEstimate(flops=10**10, bytes_accessed=2**27, transcendentals=0),
        name="plan",
    )(picks)


def weights_of(refs, penalty_ref=None):
    value = refs[0][...] if len(refs) == 1 else jnp.concatenate([r[...] for r in refs], 0)
    wide = value.astype(jnp.float32)
    top = jnp.sum(wide * wide, axis=1, keepdims=True)
    if penalty_ref is not None:
        top = top + penalty_ref[...]
    return value * jnp.bfloat16(-2.0), top


def score_kernel(number, masked, first, last, held_ref, *refs):
    rows, width = held_ref.shape
    sets = refs[:number]
    rest = list(refs[number:])
    penalty_ref = rest.pop(0) if masked else None
    if not first:
        before_ref, squares_ref = rest.pop(0), rest.pop(0)
    out_ref = rest.pop(0)
    weight, top = weights_of(sets, penalty_ref)
    ones = jnp.ones((8, 128), jnp.bfloat16)
    peak = None
    for piece in range(rows // CHUNK):
        window = pl.ds(piece * CHUNK, CHUNK)
        value = held_ref[window, :]
        part = lax.dot_general(weight, value, NT, preferred_element_type=jnp.float32)
        least = jnp.min(part + top, axis=0, keepdims=True)
        if first:
            block = value.astype(jnp.float32)
            block = block * block
            partial = block[:, :128]
            for lane in range(128, width, 128):
                partial = partial + block[:, lane : lane + 128]
            high = partial.astype(jnp.bfloat16)
            low = (partial - high.astype(jnp.float32)).astype(jnp.bfloat16)
            total = lax.dot_general(
                ones, high, NT, preferred_element_type=jnp.float32
            ) + lax.dot_general(ones, low, NT, preferred_element_type=jnp.float32)
            rest[0][:, window] = total[:1, :]
        else:
            least = jnp.minimum(least, before_ref[:, window])
        if last:
            least = (least + squares_ref[:, window]) / width
            peak = least if peak is None else jnp.maximum(peak, least)
        out_ref[:, window] = least
    if last:
        rest[0][...] = jnp.broadcast_to(jnp.max(peak, axis=1, keepdims=True), rest[0].shape)


def score(held, sets, penalty, before=None, squares=None, last=False):
    rows = held.shape[0]
    masked = penalty is not None
    first = before is None
    operands = [held, *sets] + ([penalty] if masked else [])
    out_shape = [pltpu.VMEM((1, rows), jnp.float32)]
    if first:
        out_shape.append(pltpu.VMEM((1, rows), jnp.float32))
    else:
        operands += [before, squares]
    if last:
        out_shape.append(pltpu.VMEM((8, 128), jnp.float32))
    return pl.pallas_call(
        functools.partial(score_kernel, len(sets), masked, first, last),
        out_shape=tuple(out_shape),
        in_specs=[VMEM] * len(operands),
        out_specs=(VMEM,) * len(out_shape),
        compiler_params=pltpu.CompilerParams(vmem_limit_bytes=16 * 2**20),
        cost_estimate=cost(3 * 10**9),
        name="score_first" if first else "score_last" if last else "score",
    )(*operands)


def choose(onehot, held):
    rows = held[0] if len(held) == 1 else jnp.concatenate(held, 0)
    return jnp.dot(onehot, rows, preferred_element_type=jnp.float32).astype(rows.dtype)


def phase_spans(size_gx, size_gy):
    bits_gy = size_gy.bit_length() - 1
    rounds = bits_gy + size_gx.bit_length() - 1
    spans = [(0, 1)]
    for begin, end in ((1, bits_gy), (bits_gy, rounds)):
        for step in range(begin, end, 2):
            spans.append((step, min(step + 2, end)))
    return spans


def per_device(embeddings, device_local_selections, merge_picks):
    count = device_local_selections.shape[1]
    size_gx = lax.axis_size("gx")
    size_gy = lax.axis_size("gy")
    devices = size_gx * size_gy
    number = lax.axis_index("gx") * size_gy + lax.axis_index("gy")
    north = (number & 1) == 1

    def swap(value, mask, other=None):
        other = mask if other is None else other
        pairs = [(source, source ^ (mask if source & 1 else other)) for source in range(devices)]
        return lax.ppermute(value, ("gx", "gy"), pairs)

    phases = []
    for begin, end in phase_spans(size_gx, size_gy):
        kind = "mixed" if end <= size_gy.bit_length() - 1 else "plain"
        phases.append((begin, kind if end - begin > 1 else "single"))

    sets = gather_rows(embeddings, device_local_selections)
    plan = list(make_plan(merge_picks, phases, devices))
    cover = None
    pending = None
    for step, kind in phases:
        near, high = 1 << step, 2 << step
        onehot = plan.pop(0)
        if kind == "single":
            penalty = None
            others = [swap(sets, near)]
        else:
            penalty = plan.pop(0)
            if kind == "mixed":
                half = count // 2
                part = jnp.where(north, sets[:half], sets[half:])
                first = swap(sets, near | high, near)
                second = swap(part, high)
                here = jnp.concatenate([first, second], 0)
                others = [here, swap(here, 1)]
            else:
                others = [swap(sets, near)]
                others.append(swap(sets, high))
                others.append(swap(sets, near | high))
        if pending is not None:
            if cover is None:
                cover, squares = score(embeddings, *pending)
            else:
                cover, = score(embeddings, *pending, cover, squares)
        pending = ([sets] if step == 0 else []) + others, penalty
        sets = choose(onehot, [sets] + others)
    cover, peak = score(embeddings, *pending, cover, squares, last=True)
    bit = 1
    while bit < devices:
        peak = jnp.maximum(peak, swap(peak, bit | 1))
        bit *= 2
    return (sets, cover[0], peak[0, 0])


def solution(mesh):
    return jax.shard_map(
        per_device,
        mesh=mesh,
        in_specs=(P(("gx", "gy"), None), P(("gx", "gy"), None), P()),
        out_specs=(P(), P(("gx", "gy")), P()),
        check_vma=False,
    )
```

```python
import functools

import jax
import jax.numpy as jnp
from jax import lax
from jax.experimental import pallas as pl
from jax.experimental.pallas import tpu as pltpu
from jax.sharding import PartitionSpec as P


GROUP = 8
LEGS = {"gy": ("shared", "north", "south"), "gx": ("south", "shared", "north")}
CHUNK = 256
FAR = 3.0e38
NT = (((1,), (1,)), ((), ()))
VMEM = pl.BlockSpec(memory_space=pltpu.VMEM)


def cost(flops):
    return pl.CostEstimate(flops=flops, bytes_accessed=2**20, transcendentals=0)


def gather_kernel(picks_ref, points_ref, out_ref, held, sem):
    count = out_ref.shape[0]
    copies = []
    for i in range(count):
        start = pl.multiple_of(picks_ref[0, i] // GROUP * GROUP, GROUP)
        copies.append(
            pltpu.make_async_copy(
                points_ref.at[pl.ds(start, GROUP), :],
                held.at[pl.ds(i * GROUP, GROUP), :],
                sem.at[i],
            )
        )
        copies[-1].start()
    down = lax.broadcasted_iota(jnp.int32, (count, 128), 0)
    wanted = down * GROUP
    for i in range(count):
        wanted = jnp.where(down == i, wanted + lax.rem(picks_ref[0, i], GROUP), wanted)
    lanes = lax.broadcasted_iota(jnp.int32, (count, 128), 1)
    onehot = jnp.concatenate(
        [(lanes + base == wanted).astype(jnp.bfloat16) for base in range(0, count * GROUP, 128)],
        axis=1,
    )
    for copy in copies:
        copy.wait()
    out_ref[...] = jnp.dot(
        onehot, held[...], preferred_element_type=jnp.float32
    ).astype(jnp.bfloat16)


def gather_rows(points, picks):
    count = picks.shape[1]
    width = points.shape[1]
    return pl.pallas_call(
        gather_kernel,
        out_shape=pltpu.VMEM((count, width), points.dtype),
        in_specs=[
            pl.BlockSpec(memory_space=pltpu.SMEM),
            pl.BlockSpec(memory_space=pltpu.HBM),
        ],
        out_specs=VMEM,
        scratch_shapes=[
            pltpu.VMEM((count * GROUP, width), points.dtype),
            pltpu.SemaphoreType.DMA((count,)),
        ],
        compiler_params=pltpu.CompilerParams(vmem_limit_bytes=56 * 2**20),
        cost_estimate=cost(10**9),
        name="gather_rows",
    )(picks, points)


def swap_halves(index, count, lower):
    swapped_index = jnp.where(index < count, index + count, index - count)
    return jnp.where(lower, index, swapped_index)


def upright(row):
    size = row.shape[1]
    across = lax.broadcasted_iota(jnp.int32, (size, size), 1)
    down = lax.broadcasted_iota(jnp.int32, (size, size), 0)
    spread = jnp.where(across == down, jnp.broadcast_to(row, (size, size)), 0)
    return jnp.sum(spread.astype(jnp.float32), axis=1, keepdims=True).astype(jnp.int32)


def plan_kernel(phases, count, devices, picks_ref, *out_refs):
    number = lax.axis_index("gx") * lax.axis_size("gy") + lax.axis_index("gy")
    outs = list(out_refs)
    north = (number & 1) == 1

    def row_of(step, place):
        return picks_ref[pl.ds(devices - (devices >> step) + (place >> step + 1), 1), :]

    def onehot(column, total):
        lanes = lax.broadcasted_iota(jnp.int32, (count, total), 1)
        return (lanes == column).astype(jnp.bfloat16)

    for step, kind in phases:
        lower = (number >> step & 1) == 0
        own = swap_halves(row_of(step, number), count, lower)
        if kind == "single":
            outs.pop(0)[...] = onehot(upright(own), 2 * count)
            continue
        beside = swap_halves(row_of(step, number ^ 2 << step), count, lower)
        lower_next = (number >> step + 1 & 1) == 0
        top = upright(swap_halves(row_of(step + 1, number), count, lower_next))
        lanes = lax.broadcasted_iota(jnp.int32, (count, count), 1)
        relative = jnp.where(lanes == top, own, 0) + jnp.where(
            lanes + count == top, beside + 2 * count, 0
        )
        relative = jnp.sum(relative.astype(jnp.float32), axis=1, keepdims=True)
        relative = relative.astype(jnp.int32)
        half = count // 2
        roles = [1 + LEGS[kind].index(role) for role in ("north", "south", "shared")]
        place = relative
        spot = lax.broadcasted_iota(jnp.int32, (3 * count, 1), 0)
        partner = jnp.zeros_like(spot)
        for role, low_half, start_north, start_south in (
            (roles[0], None, count, count + 3 * half),
            (roles[1], None, count + 3 * half, count),
            (roles[2], True, 2 * count, 2 * count + 3 * half),
            (roles[2], False, 2 * count + 3 * half, 2 * count),
        ):
            base = role * count + (0 if low_half in (None, True) else half)
            extent = count if low_half is None else half
            start = jnp.where(north, start_north, start_south)
            place = jnp.where(
                (relative >= base) & (relative < base + extent), relative - base + start, place
            )
            here = spot + count - start
            partner = jnp.where((here >= 0) & (here < extent), here + base, partner)
        spot = partner
        outs.pop(0)[...] = onehot(place, 4 * count)
        kept = jnp.where(spot - 2 * count == beside, 1.0, 0.0)
        kept = jnp.max(kept, axis=1, keepdims=True)
        kept = jnp.where(spot < 2 * count, 1.0, kept)
        outs.pop(0)[...] = jnp.where(kept > 0.5, 0.0, FAR)


def make_plan(picks, phases, devices):
    count = picks.shape[1]
    shapes = []
    for _, kind in phases:
        if kind == "single":
            shapes.append(pltpu.VMEM((count, 2 * count), jnp.bfloat16))
        else:
            shapes.append(pltpu.VMEM((count, 4 * count), jnp.bfloat16))
            shapes.append(pltpu.VMEM((3 * count, 1), jnp.float32))
    return pl.pallas_call(
        functools.partial(plan_kernel, phases, count, devices),
        out_shape=tuple(shapes),
        in_specs=[VMEM],
        out_specs=(VMEM,) * len(shapes),
        compiler_params=pltpu.CompilerParams(vmem_limit_bytes=4 * 2**20),
        cost_estimate=pl.CostEstimate(flops=10**10, bytes_accessed=2**27, transcendentals=0),
        name="plan",
    )(picks)


def weights_of(refs, penalty_ref=None):
    value = refs[0][...] if len(refs) == 1 else jnp.concatenate([r[...] for r in refs], 0)
    wide = value.astype(jnp.float32)
    top = jnp.sum(wide * wide, axis=1, keepdims=True)
    if penalty_ref is not None:
        top = top + penalty_ref[...]
    return value * jnp.bfloat16(-2.0), top


def score_kernel(number, masked, first, last, held_ref, *refs):
    rows, width = held_ref.shape
    sets = refs[:number]
    rest = list(refs[number:])
    penalty_ref = rest.pop(0) if masked else None
    if not first:
        before_ref, squares_ref = rest.pop(0), rest.pop(0)
    out_ref = rest.pop(0)
    weight, top = weights_of(sets, penalty_ref)
    ones = jnp.ones((8, 128), jnp.bfloat16)
    peak = None
    for piece in range(rows // CHUNK):
        window = pl.ds(piece * CHUNK, CHUNK)
        value = held_ref[window, :]
        part = lax.dot_general(weight, value, NT, preferred_element_type=jnp.float32)
        least = jnp.min(part + top, axis=0, keepdims=True)
        if first:
            block = value.astype(jnp.float32)
            block = block * block
            partial = block[:, :128]
            for lane in range(128, width, 128):
                partial = partial + block[:, lane : lane + 128]
            high = partial.astype(jnp.bfloat16)
            low = (partial - high.astype(jnp.float32)).astype(jnp.bfloat16)
            total = lax.dot_general(
                ones, high, NT, preferred_element_type=jnp.float32
            ) + lax.dot_general(ones, low, NT, preferred_element_type=jnp.float32)
            rest[0][:, window] = total[:1, :]
        else:
            least = jnp.minimum(least, before_ref[:, window])
        if last:
            least = (least + squares_ref[:, window]) / width
            peak = least if peak is None else jnp.maximum(peak, least)
        out_ref[:, window] = least
    if last:
        rest[0][...] = jnp.broadcast_to(jnp.max(peak, axis=1, keepdims=True), rest[0].shape)


def score(held, sets, penalty, before=None, squares=None, last=False):
    rows = held.shape[0]
    masked = penalty is not None
    first = before is None
    operands = [held, *sets] + ([penalty] if masked else [])
    out_shape = [pltpu.VMEM((1, rows), jnp.float32)]
    if first:
        out_shape.append(pltpu.VMEM((1, rows), jnp.float32))
    else:
        operands += [before, squares]
    if last:
        out_shape.append(pltpu.VMEM((8, 128), jnp.float32))
    return pl.pallas_call(
        functools.partial(score_kernel, len(sets), masked, first, last),
        out_shape=tuple(out_shape),
        in_specs=[VMEM] * len(operands),
        out_specs=(VMEM,) * len(out_shape),
        compiler_params=pltpu.CompilerParams(vmem_limit_bytes=16 * 2**20),
        cost_estimate=cost(3 * 10**9),
        name="score_first" if first else "score_last" if last else "score",
    )(*operands)


def choose(onehot, held):
    rows = held[0] if len(held) == 1 else jnp.concatenate(held, 0)
    return jnp.dot(onehot, rows, preferred_element_type=jnp.float32).astype(rows.dtype)


def phase_spans(size_gx, size_gy):
    bits_gy = size_gy.bit_length() - 1
    rounds = bits_gy + size_gx.bit_length() - 1
    spans = [(0, 1)]
    for begin, end in ((1, bits_gy), (bits_gy, rounds)):
        for step in range(begin, end, 2):
            spans.append((step, min(step + 2, end)))
    return spans


def per_device(embeddings, device_local_selections, merge_picks):
    count = device_local_selections.shape[1]
    size_gx = lax.axis_size("gx")
    size_gy = lax.axis_size("gy")
    devices = size_gx * size_gy
    number = lax.axis_index("gx") * size_gy + lax.axis_index("gy")
    north = (number & 1) == 1

    def swap(value, mask, other=None):
        other = mask if other is None else other
        pairs = [(source, source ^ (mask if source & 1 else other)) for source in range(devices)]
        return lax.ppermute(value, ("gx", "gy"), pairs)

    phases = []
    for begin, end in phase_spans(size_gx, size_gy):
        kind = "gy" if end <= size_gy.bit_length() - 1 else "gx"
        phases.append((begin, kind if end - begin > 1 else "single"))

    sets = gather_rows(embeddings, device_local_selections)
    plan = list(make_plan(merge_picks, phases, devices))
    cover = None
    pending = None
    for step, kind in phases:
        near, high = 1 << step, 2 << step
        onehot = plan.pop(0)
        if kind == "single":
            penalty = None
            others = [swap(sets, near)]
        else:
            penalty = plan.pop(0)
            masks = dict(zip(LEGS[kind], (near, high, near | high)))
            half = count // 2
            part = jnp.where(north, sets[:half], sets[half:])
            first = swap(sets, masks["north"], masks["south"])
            second = swap(part, masks["shared"])
            here = jnp.concatenate([first, second], 0)
            others = [here, swap(here, 1)]
        if pending is not None:
            if cover is None:
                cover, squares = score(embeddings, *pending)
            else:
                cover, = score(embeddings, *pending, cover, squares)
        pending = ([sets] if step == 0 else []) + others, penalty
        sets = choose(onehot, [sets] + others)
    cover, peak = score(embeddings, *pending, cover, squares, last=True)
    bit = 1
    while bit < devices:
        peak = jnp.maximum(peak, swap(peak, bit | 1))
        bit *= 2
    return (sets, cover[0], peak[0, 0])


def solution(mesh):
    return jax.shard_map(
        per_device,
        mesh=mesh,
        in_specs=(P(("gx", "gy"), None), P(("gx", "gy"), None), P()),
        out_specs=(P(), P(("gx", "gy")), P()),
        check_vma=False,
    )
```

```python
import functools

import jax
import jax.numpy as jnp
from jax import lax
from jax.experimental import pallas as pl
from jax.experimental.pallas import tpu as pltpu
from jax.sharding import PartitionSpec as P


GROUP = 8
LEGS = {"gy": ("shared", "north", "south"), "gx": ("south", "shared", "north")}
CHUNK = 256
NT = (((1,), (1,)), ((), ()))
VMEM = pl.BlockSpec(memory_space=pltpu.VMEM)


def cost(flops):
    return pl.CostEstimate(flops=flops, bytes_accessed=2**20, transcendentals=0)


def gather_kernel(picks_ref, points_ref, out_ref, held, sem):
    count = out_ref.shape[0]
    picks = [picks_ref[0, i] for i in range(count)]
    for i, pick in enumerate(picks):
        start = pl.multiple_of(lax.shift_right_logical(pick, 3) * GROUP, GROUP)
        pltpu.make_async_copy(
            points_ref.at[pl.ds(start, GROUP), :], held.at[pl.ds(i * GROUP, GROUP), :], sem
        ).start()
    down = lax.broadcasted_iota(jnp.int32, (count, 128), 0)
    wanted = down * GROUP
    for i, pick in enumerate(picks):
        wanted = jnp.where(down == i, wanted + (pick & (GROUP - 1)), wanted)
    lanes = lax.broadcasted_iota(jnp.int32, (count, 128), 1)
    onehot = jnp.concatenate(
        [(lanes + base == wanted).astype(jnp.bfloat16) for base in range(0, count * GROUP, 128)],
        axis=1,
    )
    pltpu.make_async_copy(points_ref.at[pl.ds(0, count * GROUP), :], held, sem).wait()
    out_ref[...] = jnp.dot(
        onehot, held[...], preferred_element_type=jnp.float32
    ).astype(jnp.bfloat16)


def gather_rows(points, picks):
    count = picks.shape[1]
    width = points.shape[1]
    return pl.pallas_call(
        gather_kernel,
        out_shape=pltpu.VMEM((count, width), points.dtype),
        in_specs=[
            pl.BlockSpec(memory_space=pltpu.SMEM),
            pl.BlockSpec(memory_space=pltpu.HBM),
        ],
        out_specs=VMEM,
        scratch_shapes=[
            pltpu.VMEM((count * GROUP, width), points.dtype),
            pltpu.SemaphoreType.DMA,
        ],
        compiler_params=pltpu.CompilerParams(vmem_limit_bytes=56 * 2**20),
        cost_estimate=cost(10**9),
        name="gather_rows",
    )(picks, points)


def swap_halves(index, count, lower):
    swapped_index = jnp.where(index < count, index + count, index - count)
    return jnp.where(lower, index, swapped_index)


def upright(row):
    size = row.shape[1]
    across = lax.broadcasted_iota(jnp.int32, (size, size), 1)
    down = lax.broadcasted_iota(jnp.int32, (size, size), 0)
    spread = jnp.where(across == down, jnp.broadcast_to(row, (size, size)), 0)
    return jnp.sum(spread.astype(jnp.float32), axis=1, keepdims=True).astype(jnp.int32)


def plan_kernel(phases, count, devices, picks_ref, *out_refs):
    number = lax.axis_index("gx") * lax.axis_size("gy") + lax.axis_index("gy")
    outs = list(out_refs)
    north = (number & 1) == 1

    def row_of(step, place):
        return picks_ref[pl.ds(devices - (devices >> step) + (place >> step + 1), 1), :]

    def onehot(column, total):
        lanes = lax.broadcasted_iota(jnp.int32, (column.shape[0], total), 1)
        return (lanes == column).astype(jnp.bfloat16)

    for step, kind in phases:
        lower = (number >> step & 1) == 0
        own = swap_halves(row_of(step, number), count, lower)
        if kind == "single":
            outs.pop(0)[...] = onehot(upright(own), 2 * count)
            continue
        beside = swap_halves(row_of(step, number ^ 2 << step), count, lower)
        lower_next = (number >> step + 1 & 1) == 0
        top = upright(swap_halves(row_of(step + 1, number), count, lower_next))
        lanes = lax.broadcasted_iota(jnp.int32, (count, count), 1)
        relative = jnp.where(lanes == top, own, 0) + jnp.where(
            lanes + count == top, beside + 2 * count, 0
        )
        relative = jnp.sum(relative.astype(jnp.float32), axis=1, keepdims=True)
        relative = relative.astype(jnp.int32)
        half = count // 2
        roles = [1 + LEGS[kind].index(role) for role in ("north", "south", "shared")]

        def placed(relative):
            place = relative
            for role, part, start_north, start_south in (
                (roles[0], None, count, count + 3 * half),
                (roles[1], None, count + 3 * half, count),
                (roles[2], 0, 2 * count, 2 * count + 3 * half),
                (roles[2], 1, 2 * count + 3 * half, 2 * count),
            ):
                base = role * count + (part or 0) * half
                extent = count if part is None else half
                inside = (relative >= base) & (relative < base + extent)
                start = jnp.where(north, start_north, start_south)
                place = jnp.where(inside, relative - base + start, place)
            return place

        outs.pop(0)[...] = onehot(placed(relative), 4 * count)
        plain = lax.broadcasted_iota(jnp.int32, (count, 1), 0) + count
        scored = jnp.concatenate([plain, upright(beside) + 2 * count], 0)
        outs.pop(0)[...] = onehot(placed(scored) - count, 3 * count)


def make_plan(picks, phases, devices):
    count = picks.shape[1]
    shapes = []
    for _, kind in phases:
        if kind == "single":
            shapes.append(pltpu.VMEM((count, 2 * count), jnp.bfloat16))
        else:
            shapes.append(pltpu.VMEM((count, 4 * count), jnp.bfloat16))
            shapes.append(pltpu.VMEM((2 * count, 3 * count), jnp.bfloat16))
    return pl.pallas_call(
        functools.partial(plan_kernel, phases, count, devices),
        out_shape=tuple(shapes),
        in_specs=[VMEM],
        out_specs=(VMEM,) * len(shapes),
        compiler_params=pltpu.CompilerParams(vmem_limit_bytes=4 * 2**20),
        cost_estimate=pl.CostEstimate(flops=10**10, bytes_accessed=2**27, transcendentals=0),
        name="plan",
    )(picks)


def prepare_kernel(points_ref, turned_ref, squares_ref):
    rows, width = points_ref.shape
    ones = jnp.ones((8, 128), jnp.bfloat16)
    down = lax.broadcasted_iota(jnp.int32, (CHUNK, CHUNK), 0)
    across = lax.broadcasted_iota(jnp.int32, (CHUNK, CHUNK), 1)
    identity = (down == across).astype(jnp.bfloat16)
    for piece in range(rows // CHUNK):
        window = pl.ds(piece * CHUNK, CHUNK)
        partial = None
        for lane in range(0, width, CHUNK):
            value = points_ref[window, pl.ds(lane, CHUNK)]
            turned_ref[pl.ds(lane, CHUNK), window] = lax.dot_general(
                identity, value, NT, preferred_element_type=jnp.float32
            ).astype(jnp.bfloat16)
            block = value.astype(jnp.float32)
            block = block * block
            for offset in range(0, CHUNK, 128):
                term = block[:, offset : offset + 128]
                partial = term if partial is None else partial + term
        high = partial.astype(jnp.bfloat16)
        low = (partial - high.astype(jnp.float32)).astype(jnp.bfloat16)
        total = lax.dot_general(
            ones, high, NT, preferred_element_type=jnp.float32
        ) + lax.dot_general(ones, low, NT, preferred_element_type=jnp.float32)
        squares_ref[:, window] = total[:1, :]


def prepare(points):
    rows, width = points.shape
    return pl.pallas_call(
        prepare_kernel,
        out_shape=(
            pltpu.VMEM((width, rows), points.dtype),
            pltpu.VMEM((1, rows), jnp.float32),
        ),
        in_specs=[VMEM],
        out_specs=(VMEM, VMEM),
        compiler_params=pltpu.CompilerParams(vmem_limit_bytes=16 * 2**20),
        cost_estimate=cost(3 * 10**9),
        name="prepare",
    )(points)


def score_kernel(shape, first, last, turned_ref, *refs):
    width, rows = turned_ref.shape
    refs = list(refs)
    values = []
    for chosen, number in shape:
        onehot = refs.pop(0)[...] if chosen else None
        value = jnp.concatenate([refs.pop(0)[...] for _ in range(number)], 0)
        if chosen:
            value = jnp.dot(onehot, value, preferred_element_type=jnp.float32)
            value = value.astype(jnp.bfloat16)
        values.append(value)
    value = values[0] if len(values) == 1 else jnp.concatenate(values, 0)
    wide = value.astype(jnp.float32)
    top = jnp.sum(wide * wide, axis=1, keepdims=True)
    weight = value * jnp.bfloat16(-2.0)
    before_ref = None if first else refs.pop(0)
    squares_ref = refs.pop(0) if last else None
    out_ref = refs.pop(0)
    peak = None
    for piece in range(rows // CHUNK):
        window = pl.ds(piece * CHUNK, CHUNK)
        part = jnp.dot(weight, turned_ref[:, window], preferred_element_type=jnp.float32)
        least = jnp.min(part + top, axis=0, keepdims=True)
        if not first:
            least = jnp.minimum(least, before_ref[:, window])
        if last:
            least = (least + squares_ref[:, window]) / width
            peak = least if peak is None else jnp.maximum(peak, least)
        out_ref[:, window] = least
    if last:
        rest = refs.pop(0)
        rest[...] = jnp.broadcast_to(jnp.max(peak, axis=1, keepdims=True), rest.shape)


def score(turned, pending, before=None, squares=None, last=False):
    rows = turned.shape[1]
    operands = [turned]
    shape = []
    for onehot, sets in pending:
        shape.append((onehot is not None, len(sets)))
        operands += ([] if onehot is None else [onehot]) + list(sets)
    if before is not None:
        operands.append(before)
    if last:
        operands.append(squares)
    out_shape = [pltpu.VMEM((1, rows), jnp.float32)]
    if last:
        out_shape.append(pltpu.VMEM((8, 128), jnp.float32))
    return pl.pallas_call(
        functools.partial(score_kernel, tuple(shape), before is None, last),
        out_shape=tuple(out_shape),
        in_specs=[VMEM] * len(operands),
        out_specs=(VMEM,) * len(out_shape),
        compiler_params=pltpu.CompilerParams(vmem_limit_bytes=16 * 2**20),
        cost_estimate=cost(3 * 10**9),
        name="score_last" if last else "score",
    )(*operands)


def choose(onehot, held):
    rows = held[0] if len(held) == 1 else jnp.concatenate(held, 0)
    return jnp.dot(onehot, rows, preferred_element_type=jnp.float32).astype(rows.dtype)


def phase_spans(size_gx, size_gy):
    bits_gy = size_gy.bit_length() - 1
    rounds = bits_gy + size_gx.bit_length() - 1
    spans = [(0, 1)]
    for begin, end in ((1, bits_gy), (bits_gy, rounds)):
        for step in range(begin, end, 2):
            spans.append((step, min(step + 2, end)))
    return spans


def per_device(embeddings, device_local_selections, merge_picks):
    count = device_local_selections.shape[1]
    size_gx = lax.axis_size("gx")
    size_gy = lax.axis_size("gy")
    devices = size_gx * size_gy
    number = lax.axis_index("gx") * size_gy + lax.axis_index("gy")
    north = (number & 1) == 1

    def swap(value, mask, other=None):
        other = mask if other is None else other
        pairs = [(source, source ^ (mask if source & 1 else other)) for source in range(devices)]
        return lax.ppermute(value, ("gx", "gy"), pairs)

    phases = []
    for begin, end in phase_spans(size_gx, size_gy):
        kind = "gy" if end <= size_gy.bit_length() - 1 else "gx"
        phases.append((begin, kind if end - begin > 1 else "single"))

    sets = gather_rows(embeddings, device_local_selections)
    plan = list(make_plan(merge_picks, phases, devices))
    cover = None
    pending = []
    for place, (step, kind) in enumerate(phases):
        near, high = 1 << step, 2 << step
        onehot = plan.pop(0)
        if kind == "single":
            kept = None
            others = [swap(sets, near)]
        else:
            kept = plan.pop(0)
            masks = dict(zip(LEGS[kind], (near, high, near | high)))
            half = count // 2
            part = jnp.where(north, sets[:half], sets[half:])
            first = swap(sets, masks["north"], masks["south"])
            second = swap(part, masks["shared"])
            here = jnp.concatenate([first, second], 0)
            others = [here, swap(here, 1)]
        if place == 1:
            turned, squares = prepare(embeddings)
        elif place > 1:
            (cover,) = score(turned, pending, cover)
            pending = []
        pending.append((kept, ([sets] if step == 0 else []) + others))
        sets = choose(onehot, [sets] + others)
    cover, peak = score(turned, pending, cover, squares, last=True)
    bit = 1
    while bit < devices:
        peak = jnp.maximum(peak, swap(peak, bit | 1))
        bit *= 2
    return (sets, cover[0], peak[0, 0])


def solution(mesh):
    return jax.shard_map(
        per_device,
        mesh=mesh,
        in_specs=(P(("gx", "gy"), None), P(("gx", "gy"), None), P()),
        out_specs=(P(), P(("gx", "gy")), P()),
        check_vma=False,
    )
```

```python
import functools

import jax
import jax.numpy as jnp
from jax import lax
from jax.experimental import pallas as pl
from jax.experimental.pallas import tpu as pltpu
from jax.sharding import PartitionSpec as P


GROUP = 8
LEGS = {"gy": ("south", "north", "shared"), "gx": ('south', 'shared', 'north')}
CHUNK = 256
NT = (((1,), (1,)), ((), ()))
VMEM = pl.BlockSpec(memory_space=pltpu.VMEM)


def cost(flops):
    return pl.CostEstimate(flops=flops, bytes_accessed=2**20, transcendentals=0)


def gather_kernel(picks_ref, points_ref, out_ref, held, sem):
    count = out_ref.shape[0]
    picks = [picks_ref[0, i] for i in range(count)]
    for i, pick in enumerate(picks):
        start = pl.multiple_of(lax.shift_right_logical(pick, 3) * GROUP, GROUP)
        pltpu.make_async_copy(
            points_ref.at[pl.ds(start, GROUP), :], held.at[pl.ds(i * GROUP, GROUP), :], sem
        ).start()
    down = lax.broadcasted_iota(jnp.int32, (count, 128), 0)
    wanted = down * GROUP
    for i, pick in enumerate(picks):
        wanted = jnp.where(down == i, wanted + (pick & (GROUP - 1)), wanted)
    lanes = lax.broadcasted_iota(jnp.int32, (count, 128), 1)
    onehot = jnp.concatenate(
        [(lanes + base == wanted).astype(jnp.bfloat16) for base in range(0, count * GROUP, 128)],
        axis=1,
    )
    pltpu.make_async_copy(points_ref.at[pl.ds(0, count * GROUP), :], held, sem).wait()
    out_ref[...] = jnp.dot(
        onehot, held[...], preferred_element_type=jnp.float32
    ).astype(jnp.bfloat16)


def gather_rows(points, picks):
    count = picks.shape[1]
    width = points.shape[1]
    return pl.pallas_call(
        gather_kernel,
        out_shape=pltpu.VMEM((count, width), points.dtype),
        in_specs=[
            pl.BlockSpec(memory_space=pltpu.SMEM),
            pl.BlockSpec(memory_space=pltpu.HBM),
        ],
        out_specs=VMEM,
        scratch_shapes=[
            pltpu.VMEM((count * GROUP, width), points.dtype),
            pltpu.SemaphoreType.DMA,
        ],
        compiler_params=pltpu.CompilerParams(vmem_limit_bytes=56 * 2**20),
        cost_estimate=cost(10**9),
        name="gather_rows",
    )(picks, points)


def swap_halves(index, count, lower):
    swapped_index = jnp.where(index < count, index + count, index - count)
    return jnp.where(lower, index, swapped_index)


def upright(row):
    size = row.shape[1]
    across = lax.broadcasted_iota(jnp.int32, (size, size), 1)
    down = lax.broadcasted_iota(jnp.int32, (size, size), 0)
    spread = jnp.where(across == down, jnp.broadcast_to(row, (size, size)), 0)
    return jnp.sum(spread.astype(jnp.float32), axis=1, keepdims=True).astype(jnp.int32)


def plan_kernel(phases, count, devices, picks_ref, *out_refs):
    number = lax.axis_index("gx") * lax.axis_size("gy") + lax.axis_index("gy")
    outs = list(out_refs)
    north = (number & 1) == 1

    def row_of(step, place):
        return picks_ref[pl.ds(devices - (devices >> step) + (place >> step + 1), 1), :]

    def onehot(column, total):
        lanes = lax.broadcasted_iota(jnp.int32, (column.shape[0], total), 1)
        return (lanes == column).astype(jnp.bfloat16)

    for step, kind in phases:
        lower = (number >> step & 1) == 0
        own = swap_halves(row_of(step, number), count, lower)
        if kind == "single":
            outs.pop(0)[...] = onehot(upright(own), 2 * count)
            continue
        beside = swap_halves(row_of(step, number ^ 2 << step), count, lower)
        lower_next = (number >> step + 1 & 1) == 0
        top = upright(swap_halves(row_of(step + 1, number), count, lower_next))
        lanes = lax.broadcasted_iota(jnp.int32, (count, count), 1)
        relative = jnp.where(lanes == top, own, 0) + jnp.where(
            lanes + count == top, beside + 2 * count, 0
        )
        relative = jnp.sum(relative.astype(jnp.float32), axis=1, keepdims=True)
        relative = relative.astype(jnp.int32)
        half = count // 2
        roles = [1 + LEGS[kind].index(role) for role in ("north", "south", "shared")]

        def placed(relative):
            place = relative
            for role, part, start_north, start_south in (
                (roles[0], None, count, count + 3 * half),
                (roles[1], None, count + 3 * half, count),
                (roles[2], 0, 2 * count, 2 * count + 3 * half),
                (roles[2], 1, 2 * count + 3 * half, 2 * count),
            ):
                base = role * count + (part or 0) * half
                extent = count if part is None else half
                inside = (relative >= base) & (relative < base + extent)
                start = jnp.where(north, start_north, start_south)
                place = jnp.where(inside, relative - base + start, place)
            return place

        outs.pop(0)[...] = onehot(placed(relative), 4 * count)
        plain = lax.broadcasted_iota(jnp.int32, (count, 1), 0) + count
        scored = jnp.concatenate([plain, upright(beside) + 2 * count], 0)
        outs.pop(0)[...] = onehot(placed(scored) - count, 3 * count)


def make_plan(picks, phases, devices):
    count = picks.shape[1]
    shapes = []
    for _, kind in phases:
        if kind == "single":
            shapes.append(pltpu.VMEM((count, 2 * count), jnp.bfloat16))
        else:
            shapes.append(pltpu.VMEM((count, 4 * count), jnp.bfloat16))
            shapes.append(pltpu.VMEM((2 * count, 3 * count), jnp.bfloat16))
    return pl.pallas_call(
        functools.partial(plan_kernel, phases, count, devices),
        out_shape=tuple(shapes),
        in_specs=[VMEM],
        out_specs=(VMEM,) * len(shapes),
        compiler_params=pltpu.CompilerParams(vmem_limit_bytes=4 * 2**20),
        cost_estimate=pl.CostEstimate(flops=10**10, bytes_accessed=2**27, transcendentals=0),
        name="plan",
    )(picks)


def prepare_kernel(points_ref, turned_ref, squares_ref):
    rows, width = points_ref.shape
    ones = jnp.ones((8, 128), jnp.bfloat16)
    down = lax.broadcasted_iota(jnp.int32, (CHUNK, CHUNK), 0)
    across = lax.broadcasted_iota(jnp.int32, (CHUNK, CHUNK), 1)
    identity = (down == across).astype(jnp.bfloat16)
    for piece in range(rows // CHUNK):
        window = pl.ds(piece * CHUNK, CHUNK)
        partial = None
        for lane in range(0, width, CHUNK):
            value = points_ref[window, pl.ds(lane, CHUNK)]
            turned_ref[pl.ds(lane, CHUNK), window] = lax.dot_general(
                identity, value, NT, preferred_element_type=jnp.float32
            ).astype(jnp.bfloat16)
            block = value.astype(jnp.float32)
            block = block * block
            for offset in range(0, CHUNK, 128):
                term = block[:, offset : offset + 128]
                partial = term if partial is None else partial + term
        high = partial.astype(jnp.bfloat16)
        low = (partial - high.astype(jnp.float32)).astype(jnp.bfloat16)
        total = lax.dot_general(
            ones, high, NT, preferred_element_type=jnp.float32
        ) + lax.dot_general(ones, low, NT, preferred_element_type=jnp.float32)
        squares_ref[:, window] = total[:1, :]


def prepare(points):
    rows, width = points.shape
    return pl.pallas_call(
        prepare_kernel,
        out_shape=(
            pltpu.VMEM((width, rows), points.dtype),
            pltpu.VMEM((1, rows), jnp.float32),
        ),
        in_specs=[VMEM],
        out_specs=(VMEM, VMEM),
        compiler_params=pltpu.CompilerParams(vmem_limit_bytes=16 * 2**20),
        cost_estimate=cost(3 * 10**9),
        name="prepare",
    )(points)


def score_kernel(shape, first, last, turned_ref, *refs):
    width, rows = turned_ref.shape
    refs = list(refs)
    values = []
    raw = []
    for chosen, number in shape:
        onehot = refs.pop(0)[...] if chosen else None
        raw.append([refs.pop(0) for _ in range(number)])
        value = jnp.concatenate([ref[...] for ref in raw[-1]], 0)
        if chosen:
            value = jnp.dot(onehot, value, preferred_element_type=jnp.float32)
            value = value.astype(jnp.bfloat16)
        values.append(value)
    value = values[0] if len(values) == 1 else jnp.concatenate(values, 0)
    wide = value.astype(jnp.float32)
    top = jnp.sum(wide * wide, axis=1, keepdims=True)
    weight = value * jnp.bfloat16(-2.0)
    before_ref = None if first else refs.pop(0)
    squares_ref = refs.pop(0) if last else None
    if last:
        onehot_ref, own_ref, out_ref, sets_ref, peak_ref = refs
        held = jnp.concatenate([own_ref[...]] + [ref[...] for ref in raw[-1]], 0)
        sets_ref[...] = jnp.dot(
            onehot_ref[...], held, preferred_element_type=jnp.float32
        ).astype(jnp.bfloat16)
    else:
        out_ref = refs.pop(0)
    peak = None
    for piece in range(rows // CHUNK):
        window = pl.ds(piece * CHUNK, CHUNK)
        part = jnp.dot(weight, turned_ref[:, window], preferred_element_type=jnp.float32)
        least = jnp.min(part + top, axis=0, keepdims=True)
        if not first:
            least = jnp.minimum(least, before_ref[:, window])
        if last:
            least = (least + squares_ref[:, window]) / width
            peak = least if peak is None else jnp.maximum(peak, least)
        out_ref[:, window] = least
    if last:
        most = jnp.max(peak, axis=1, keepdims=True)
        peak_ref[...] = jnp.broadcast_to(most[None], peak_ref.shape)


def score(turned, pending, before=None, squares=None, final=None, devices=0):
    _, rows = turned.shape
    operands = [turned]
    shape = []
    for onehot, sets in pending:
        shape.append((onehot is not None, len(sets)))
        operands += ([] if onehot is None else [onehot]) + list(sets)
    if before is not None:
        operands.append(before)
    last = final is not None
    out_shape = [pltpu.VMEM((1, rows), jnp.float32)]
    if last:
        operands += [squares, *final]
        out_shape += [
            pltpu.VMEM(final[1].shape, turned.dtype),
            pltpu.VMEM((devices, 1, 128), jnp.float32),
        ]
    return pl.pallas_call(
        functools.partial(score_kernel, tuple(shape), before is None, last),
        out_shape=tuple(out_shape),
        in_specs=[VMEM] * len(operands),
        out_specs=(VMEM,) * len(out_shape),
        compiler_params=pltpu.CompilerParams(vmem_limit_bytes=16 * 2**20),
        cost_estimate=cost(3 * 10**9),
        name="score_last" if last else "score",
    )(*operands)


def finish_kernel(peaks_ref, cover_ref, sets_ref, cover_out, sets_out, radius_out, radius, sems):
    radius[...] = jnp.max(jnp.max(peaks_ref[...], axis=0), axis=1, keepdims=True)
    copies = [
        pltpu.make_async_copy(source, target, sems.at[place])
        for place, (source, target) in enumerate(
            ((cover_ref, cover_out), (sets_ref, sets_out), (radius, radius_out))
        )
    ]
    for copy in copies:
        copy.start()
    for copy in copies:
        copy.wait()


def finish(peaks, cover, sets):
    hbm = pl.BlockSpec(memory_space=pltpu.HBM)
    return pl.pallas_call(
        finish_kernel,
        out_shape=(
            jax.ShapeDtypeStruct(cover.shape, cover.dtype),
            jax.ShapeDtypeStruct(sets.shape, sets.dtype),
            jax.ShapeDtypeStruct((1, 1), jnp.float32),
        ),
        in_specs=[VMEM] * 3,
        out_specs=(hbm, hbm, hbm),
        scratch_shapes=[pltpu.VMEM((1, 1), jnp.float32), pltpu.SemaphoreType.DMA((3,))],
        compiler_params=pltpu.CompilerParams(vmem_limit_bytes=4 * 2**20),
        name="finish",
    )(peaks, cover, sets)


def choose(onehot, held):
    rows = held[0] if len(held) == 1 else jnp.concatenate(held, 0)
    return jnp.dot(onehot, rows, preferred_element_type=jnp.float32).astype(rows.dtype)


def phase_spans(size_gx, size_gy):
    bits_gy = size_gy.bit_length() - 1
    rounds = bits_gy + size_gx.bit_length() - 1
    spans = [(0, 1)]
    for begin, end in ((1, bits_gy), (bits_gy, rounds)):
        for step in range(begin, end, 2):
            spans.append((step, min(step + 2, end)))
    return spans


def per_device(embeddings, device_local_selections, merge_picks):
    count = device_local_selections.shape[1]
    size_gx = lax.axis_size("gx")
    size_gy = lax.axis_size("gy")
    devices = size_gx * size_gy
    number = lax.axis_index("gx") * size_gy + lax.axis_index("gy")
    north = (number & 1) == 1

    def swap(value, mask, other=None):
        other = mask if other is None else other
        pairs = [(source, source ^ (mask if source & 1 else other)) for source in range(devices)]
        return lax.ppermute(value, ("gx", "gy"), pairs)

    phases = []
    for begin, end in phase_spans(size_gx, size_gy):
        kind = "gy" if end <= size_gy.bit_length() - 1 else "gx"
        phases.append((begin, kind if end - begin > 1 else "single"))

    sets = gather_rows(embeddings, device_local_selections)
    plan = list(make_plan(merge_picks, phases, devices))
    cover = None
    pending = []
    for place, (step, kind) in enumerate(phases):
        near, high = 1 << step, 2 << step
        onehot = plan.pop(0)
        if kind == "single":
            kept = None
            others = [swap(sets, near)]
        else:
            kept = plan.pop(0)
            masks = dict(zip(LEGS[kind], (near, high, near | high)))
            half = count // 2
            part = jnp.where(north, sets[:half], sets[half:])
            first = swap(sets, masks["north"], masks["south"])
            second = swap(part, masks["shared"])
            here = jnp.concatenate([first, second], 0)
            others = [here, swap(here, 1)]
        if place == 1:
            turned, squares = prepare(embeddings)
        elif place > 1:
            (cover,) = score(turned, pending, cover)
            pending = []
        pending.append((kept, ([sets] if step == 0 else []) + others))
        if place + 1 < len(phases):
            sets = choose(onehot, [sets] + others)
    cover, sets, peak = score(turned, pending, cover, squares, (onehot, sets), devices)
    peak = lax.all_to_all(peak, ("gx", "gy"), 0, 0, tiled=True)
    cover, sets, radius = finish(peak, cover, sets)
    return (sets, cover[0], radius[0, 0])


def solution(mesh):
    return jax.shard_map(
        per_device,
        mesh=mesh,
        in_specs=(P(("gx", "gy"), None), P(("gx", "gy"), None), P()),
        out_specs=(P(), P(("gx", "gy")), P()),
        check_vma=False,
    )
```

```python
import functools

import jax
import jax.numpy as jnp
from jax import lax
from jax.experimental import pallas as pl
from jax.experimental.pallas import tpu as pltpu
from jax.sharding import PartitionSpec as P


GROUP = 8
LEGS = {"gy": ("south", "north", "shared"), "gx": ('south', 'shared', 'north')}
CHUNK = 256
NT = (((1,), (1,)), ((), ()))
VMEM = pl.BlockSpec(memory_space=pltpu.VMEM)


def cost(flops):
    return pl.CostEstimate(flops=flops, bytes_accessed=2**20, transcendentals=0)


def gather_kernel(picks_ref, points_ref, out_ref, held, sem):
    count = out_ref.shape[0]
    picks = [picks_ref[0, i] for i in range(count)]
    for i, pick in enumerate(picks):
        start = pl.multiple_of(lax.shift_right_logical(pick, 3) * GROUP, GROUP)
        pltpu.make_async_copy(
            points_ref.at[pl.ds(start, GROUP), :], held.at[pl.ds(i * GROUP, GROUP), :], sem
        ).start()
    down = lax.broadcasted_iota(jnp.int32, (count, 128), 0)
    wanted = down * GROUP
    for i, pick in enumerate(picks):
        wanted = jnp.where(down == i, wanted + (pick & (GROUP - 1)), wanted)
    lanes = lax.broadcasted_iota(jnp.int32, (count, 128), 1)
    onehot = jnp.concatenate(
        [(lanes + base == wanted).astype(jnp.bfloat16) for base in range(0, count * GROUP, 128)],
        axis=1,
    )
    pltpu.make_async_copy(points_ref.at[pl.ds(0, count * GROUP), :], held, sem).wait()
    out_ref[...] = jnp.dot(
        onehot, held[...], preferred_element_type=jnp.float32
    ).astype(jnp.bfloat16)


def gather_rows(points, picks):
    count = picks.shape[1]
    width = points.shape[1]
    return pl.pallas_call(
        gather_kernel,
        out_shape=pltpu.VMEM((count, width), points.dtype),
        in_specs=[
            pl.BlockSpec(memory_space=pltpu.SMEM),
            pl.BlockSpec(memory_space=pltpu.HBM),
        ],
        out_specs=VMEM,
        scratch_shapes=[
            pltpu.VMEM((count * GROUP, width), points.dtype),
            pltpu.SemaphoreType.DMA,
        ],
        compiler_params=pltpu.CompilerParams(vmem_limit_bytes=56 * 2**20),
        cost_estimate=cost(10**9),
        name="gather_rows",
    )(picks, points)


def swap_halves(index, count, lower):
    swapped_index = jnp.where(index < count, index + count, index - count)
    return jnp.where(lower, index, swapped_index)


def upright(row):
    size = row.shape[1]
    across = lax.broadcasted_iota(jnp.int32, (size, size), 1)
    down = lax.broadcasted_iota(jnp.int32, (size, size), 0)
    spread = jnp.where(across == down, jnp.broadcast_to(row, (size, size)), 0)
    return jnp.sum(spread.astype(jnp.float32), axis=1, keepdims=True).astype(jnp.int32)


def plan_kernel(phases, count, devices, picks_ref, *out_refs):
    number = lax.axis_index("gx") * lax.axis_size("gy") + lax.axis_index("gy")
    outs = list(out_refs)
    north = (number & 1) == 1

    def row_of(step, place):
        return picks_ref[pl.ds(devices - (devices >> step) + (place >> step + 1), 1), :]

    def onehot(column, total):
        lanes = lax.broadcasted_iota(jnp.int32, (column.shape[0], total), 1)
        return (lanes == column).astype(jnp.bfloat16)

    for step, kind in phases:
        lower = (number >> step & 1) == 0
        own = swap_halves(row_of(step, number), count, lower)
        if kind == "single":
            outs.pop(0)[...] = onehot(upright(own), 2 * count)
            continue
        beside = swap_halves(row_of(step, number ^ 2 << step), count, lower)
        lower_next = (number >> step + 1 & 1) == 0
        top = upright(swap_halves(row_of(step + 1, number), count, lower_next))
        lanes = lax.broadcasted_iota(jnp.int32, (count, count), 1)
        relative = jnp.where(lanes == top, own, 0) + jnp.where(
            lanes + count == top, beside + 2 * count, 0
        )
        relative = jnp.sum(relative.astype(jnp.float32), axis=1, keepdims=True)
        relative = relative.astype(jnp.int32)
        half = count // 2
        roles = [1 + LEGS[kind].index(role) for role in ("north", "south", "shared")]

        def placed(relative):
            place = relative
            for role, part, start_north, start_south in (
                (roles[0], None, count, count + 3 * half),
                (roles[1], None, count + 3 * half, count),
                (roles[2], 0, 2 * count, 2 * count + 3 * half),
                (roles[2], 1, 2 * count + 3 * half, 2 * count),
            ):
                base = role * count + (part or 0) * half
                extent = count if part is None else half
                inside = (relative >= base) & (relative < base + extent)
                start = jnp.where(north, start_north, start_south)
                place = jnp.where(inside, relative - base + start, place)
            return place

        outs.pop(0)[...] = onehot(placed(relative), 4 * count)
        plain = lax.broadcasted_iota(jnp.int32, (count, 1), 0) + count
        scored = jnp.concatenate([plain, upright(beside) + 2 * count], 0)
        outs.pop(0)[...] = onehot(placed(scored) - count, 3 * count)


def make_plan(picks, phases, devices):
    count = picks.shape[1]
    shapes = []
    for _, kind in phases:
        if kind == "single":
            shapes.append(pltpu.VMEM((count, 2 * count), jnp.bfloat16))
        else:
            shapes.append(pltpu.VMEM((count, 4 * count), jnp.bfloat16))
            shapes.append(pltpu.VMEM((2 * count, 3 * count), jnp.bfloat16))
    return pl.pallas_call(
        functools.partial(plan_kernel, phases, count, devices),
        out_shape=tuple(shapes),
        in_specs=[VMEM],
        out_specs=(VMEM,) * len(shapes),
        compiler_params=pltpu.CompilerParams(vmem_limit_bytes=4 * 2**20),
        cost_estimate=pl.CostEstimate(flops=10**10, bytes_accessed=2**27, transcendentals=0),
        name="plan",
    )(picks)


def prepare_kernel(points_ref, turned_ref, squares_ref):
    rows, width = points_ref.shape
    ones = jnp.ones((8, 128), jnp.bfloat16)
    down = lax.broadcasted_iota(jnp.int32, (CHUNK, CHUNK), 0)
    across = lax.broadcasted_iota(jnp.int32, (CHUNK, CHUNK), 1)
    identity = (down == across).astype(jnp.bfloat16)
    for piece in range(rows // CHUNK):
        window = pl.ds(piece * CHUNK, CHUNK)
        partial = None
        for lane in range(0, width, CHUNK):
            value = points_ref[window, pl.ds(lane, CHUNK)]
            turned_ref[pl.ds(lane, CHUNK), window] = lax.dot_general(
                identity, value, NT, preferred_element_type=jnp.float32
            ).astype(jnp.bfloat16)
            block = value.astype(jnp.float32)
            block = block * block
            for offset in range(0, CHUNK, 128):
                term = block[:, offset : offset + 128]
                partial = term if partial is None else partial + term
        high = partial.astype(jnp.bfloat16)
        low = (partial - high.astype(jnp.float32)).astype(jnp.bfloat16)
        total = lax.dot_general(
            ones, high, NT, preferred_element_type=jnp.float32
        ) + lax.dot_general(ones, low, NT, preferred_element_type=jnp.float32)
        squares_ref[:, window] = total[:1, :]


def prepare(points):
    rows, width = points.shape
    return pl.pallas_call(
        prepare_kernel,
        out_shape=(
            pltpu.VMEM((width, rows), points.dtype),
            pltpu.VMEM((1, rows), jnp.float32),
        ),
        in_specs=[VMEM],
        out_specs=(VMEM, VMEM),
        compiler_params=pltpu.CompilerParams(vmem_limit_bytes=16 * 2**20),
        cost_estimate=cost(3 * 10**9),
        name="prepare",
    )(points)


def score_kernel(shape, first, last, turned_ref, *refs):
    width, rows = turned_ref.shape
    refs = list(refs)
    values = []
    raw = []
    for chosen, number in shape:
        onehot = refs.pop(0)[...] if chosen else None
        raw.append([refs.pop(0) for _ in range(number)])
        value = jnp.concatenate([ref[...] for ref in raw[-1]], 0)
        if chosen:
            value = jnp.dot(onehot, value, preferred_element_type=jnp.float32)
            value = value.astype(jnp.bfloat16)
        values.append(value)
    value = values[0] if len(values) == 1 else jnp.concatenate(values, 0)
    wide = value.astype(jnp.float32)
    top = jnp.sum(wide * wide, axis=1, keepdims=True)
    weight = value * jnp.bfloat16(-2.0)
    before_ref = None if first else refs.pop(0)
    squares_ref = refs.pop(0) if last else None
    if last:
        onehot_ref, own_ref, out_ref, sets_out, peak_ref, sets_ref, sem = refs
        sets_copy = pltpu.make_async_copy(sets_ref, sets_out, sem)
        held = jnp.concatenate([own_ref[...]] + [ref[...] for ref in raw[-1]], 0)
        sets_ref[...] = jnp.dot(
            onehot_ref[...], held, preferred_element_type=jnp.float32
        ).astype(jnp.bfloat16)
    else:
        out_ref = refs.pop(0)
    peak = None
    for piece in range(rows // CHUNK):
        window = pl.ds(piece * CHUNK, CHUNK)
        part = jnp.dot(weight, turned_ref[:, window], preferred_element_type=jnp.float32)
        least = jnp.min(part + top, axis=0, keepdims=True)
        if not first:
            least = jnp.minimum(least, before_ref[:, window])
        if last:
            least = (least + squares_ref[:, window]) / width
            peak = least if peak is None else jnp.maximum(peak, least)
        out_ref[:, window] = least
        if last and piece == 1:
            sets_copy.start()
    if last:
        sets_copy.wait()
        most = jnp.max(peak, axis=1, keepdims=True)
        peak_ref[...] = jnp.broadcast_to(most[None], peak_ref.shape)


def score(turned, pending, before=None, squares=None, final=None, devices=0):
    _, rows = turned.shape
    operands = [turned]
    shape = []
    for onehot, sets in pending:
        shape.append((onehot is not None, len(sets)))
        operands += ([] if onehot is None else [onehot]) + list(sets)
    if before is not None:
        operands.append(before)
    last = final is not None
    out_shape = [pltpu.VMEM((1, rows), jnp.float32)]
    if last:
        operands += [squares, *final]
        out_shape += [
            jax.ShapeDtypeStruct(final[1].shape, turned.dtype),
            pltpu.VMEM((devices, 1, 128), jnp.float32),
        ]
    return pl.pallas_call(
        functools.partial(score_kernel, tuple(shape), before is None, last),
        out_shape=tuple(out_shape),
        in_specs=[VMEM] * len(operands),
        out_specs=(VMEM, pl.BlockSpec(memory_space=pltpu.HBM), VMEM) if last else (VMEM,),
        scratch_shapes=[pltpu.VMEM(final[1].shape, turned.dtype), pltpu.SemaphoreType.DMA]
        if last
        else [],
        compiler_params=pltpu.CompilerParams(vmem_limit_bytes=16 * 2**20),
        cost_estimate=cost(3 * 10**9),
        name="score_last" if last else "score",
    )(*operands)


def finish_kernel(peaks_ref, cover_ref, cover_out, radius_out, radius, sems):
    radius[...] = jnp.max(jnp.max(peaks_ref[...], axis=0), axis=1, keepdims=True)
    copies = [
        pltpu.make_async_copy(source, target, sems.at[place])
        for place, (source, target) in enumerate(
            ((cover_ref, cover_out), (radius, radius_out))
        )
    ]
    for copy in copies:
        copy.start()
    for copy in copies:
        copy.wait()


def finish(peaks, cover):
    hbm = pl.BlockSpec(memory_space=pltpu.HBM)
    return pl.pallas_call(
        finish_kernel,
        out_shape=(
            jax.ShapeDtypeStruct(cover.shape, cover.dtype),
            jax.ShapeDtypeStruct((1, 1), jnp.float32),
        ),
        in_specs=[VMEM] * 2,
        out_specs=(hbm, hbm),
        scratch_shapes=[pltpu.VMEM((1, 1), jnp.float32), pltpu.SemaphoreType.DMA((2,))],
        compiler_params=pltpu.CompilerParams(vmem_limit_bytes=4 * 2**20),
        name="finish",
    )(peaks, cover)


def choose(onehot, held):
    rows = held[0] if len(held) == 1 else jnp.concatenate(held, 0)
    return jnp.dot(onehot, rows, preferred_element_type=jnp.float32).astype(rows.dtype)


def phase_spans(size_gx, size_gy):
    bits_gy = size_gy.bit_length() - 1
    rounds = bits_gy + size_gx.bit_length() - 1
    spans = [(0, 1)]
    for begin, end in ((1, bits_gy), (bits_gy, rounds)):
        for step in range(begin, end, 2):
            spans.append((step, min(step + 2, end)))
    return spans


def per_device(embeddings, device_local_selections, merge_picks):
    count = device_local_selections.shape[1]
    size_gx = lax.axis_size("gx")
    size_gy = lax.axis_size("gy")
    devices = size_gx * size_gy
    number = lax.axis_index("gx") * size_gy + lax.axis_index("gy")
    north = (number & 1) == 1

    def swap(value, mask, other=None):
        other = mask if other is None else other
        pairs = [(source, source ^ (mask if source & 1 else other)) for source in range(devices)]
        return lax.ppermute(value, ("gx", "gy"), pairs)

    phases = []
    for begin, end in phase_spans(size_gx, size_gy):
        kind = "gy" if end <= size_gy.bit_length() - 1 else "gx"
        phases.append((begin, kind if end - begin > 1 else "single"))

    sets = gather_rows(embeddings, device_local_selections)
    plan = list(make_plan(merge_picks, phases, devices))
    cover = None
    pending = []
    for place, (step, kind) in enumerate(phases):
        near, high = 1 << step, 2 << step
        onehot = plan.pop(0)
        if kind == "single":
            kept = None
            others = [swap(sets, near)]
        else:
            kept = plan.pop(0)
            masks = dict(zip(LEGS[kind], (near, high, near | high)))
            half = count // 2
            part = jnp.where(north, sets[:half], sets[half:])
            first = swap(sets, masks["north"], masks["south"])
            second = swap(part, masks["shared"])
            here = jnp.concatenate([first, second], 0)
            others = [here, swap(here, 1)]
        if place == 1:
            turned, squares = prepare(embeddings)
        elif place > 1:
            (cover,) = score(turned, pending, cover)
            pending = []
        pending.append((kept, ([sets] if step == 0 else []) + others))
        if place + 1 < len(phases):
            sets = choose(onehot, [sets] + others)
    cover, sets, peak = score(turned, pending, cover, squares, (onehot, sets), devices)
    peak = lax.all_to_all(peak, ("gx", "gy"), 0, 0, tiled=True)
    cover, radius = finish(peak, cover)
    return (sets, cover[0], radius[0, 0])


def solution(mesh):
    return jax.shard_map(
        per_device,
        mesh=mesh,
        in_specs=(P(("gx", "gy"), None), P(("gx", "gy"), None), P()),
        out_specs=(P(), P(("gx", "gy")), P()),
        check_vma=False,
    )
```
